128 devices in a mesh: dp: 16 (over x, y_hi, core), tensor: 8 (over y_lo, z).
Axes of the slice: x: 4, y: 4 (y_hi: 2, y_lo: 2; y = y_hi * 2 + y_lo), z: 4, core: 2. Of those that a mesh axis runs over, the one named last changes fastest.
Arguments:
- grad_out: bfloat16 [4096, 4096], P('dp'), may hold values from -6 to 6
- down_weight: bfloat16 [14336, 4096], P('tensor'), may hold values from -0.046875 to 0.046875
- gate_pre: bfloat16 [4096, 14336], P('dp', 'tensor'), may hold values from -8 to 8
- up_pre: bfloat16 [4096, 14336], P('dp', 'tensor'), may hold values from -6 to 6
Outputs:
- factor: float32 [14336, 14336], P('dp', 'tensor')
- grad_up: bfloat16 [4096, 14336], P('dp', 'tensor')
The draws below stay inside these ranges and needn't reach their ends.
All inputs are finite; a program needn't handle non-finite values.
Results may differ from the reference program's by a relative error of at most 0.0046.
Values may be sent and summed in bfloat16 or wider, within the bound.
A program may use at most 128 MiB of HBM per device.

```python
import jax
import jax.numpy as jnp

D = 4096
FF = 14336
TOKENS = 4096


def steps_of(key, dims, shards, low, largest):
    factor_of = 1.0
    for dim, parts in shards:
        heights = jax.random.uniform(jax.random.fold_in(jax.random.fold_in(key, 6), dim), (parts,), jnp.float32, low / len(shards), largest / len(shards))
        factor_of = factor_of * jnp.repeat(jnp.exp(heights), dims[dim] // parts).reshape((-1,) + (1,) * (len(dims) - 1 - dim))
    return factor_of


def centred(rng, shape, deviation, reach, cuts=(), held_as=jnp.bfloat16):
    array = deviation * jax.random.normal(rng, shape, jnp.float32)
    if cuts:
        array = array * steps_of(rng, shape, cuts, -0.22, 0.18)
    return jnp.clip(array, -reach, reach).astype(held_as)


def setup_inputs(seed: int = 0) -> dict:
    splits = jax.random.split(jax.random.key(seed), 5)
    return {
        "grad_out": centred(splits[0], (TOKENS, D), 1.0, 6.0, ((0, 16),)),
        "down_weight": centred(splits[1], (FF, D), FF ** -0.5, 0.046875, ((0, 8),)),
        "gate_pre": centred(splits[2], (TOKENS, FF), 1.5, 8.0, ((0, 16), (1, 8))),
        "up_pre": centred(splits[3], (TOKENS, FF), 1.0, 6.0, ((0, 16), (1, 8))),
    }


def reference(grad_out, down_weight, gate_pre, up_pre):
    hidden_grad = jnp.dot(grad_out, down_weight.T, preferred_element_type=jnp.float32)
    gate_value = gate_pre.astype(jnp.float32)
    sigmoid_gate = jax.nn.sigmoid(gate_value)
    silu_slope = sigmoid_gate * (1.0 + gate_value * (1.0 - sigmoid_gate))
    grad_gate = (hidden_grad * up_pre.astype(jnp.float32) * silu_slope).astype(jnp.bfloat16)
    grad_up = (hidden_grad * gate_value * sigmoid_gate).astype(jnp.bfloat16)
    factor = jnp.dot(grad_gate.T, grad_gate, preferred_element_type=jnp.float32) / jnp.float32(TOKENS)
    return factor, grad_up
```

```python
import jax
import jax.numpy as jnp
from jax import lax
from jax.sharding import PartitionSpec as P


def local(grad_out, down_weight, gate_pre, up_pre):
    hidden_grad = lax.dot_general(
        grad_out, down_weight, (((1,), (1,)), ((), ())), preferred_element_type=jnp.float32
    )
    gate_value = gate_pre.astype(jnp.float32)
    sigmoid_gate = jax.nn.sigmoid(gate_value)
    silu_slope = sigmoid_gate * (1.0 + gate_value * (1.0 - sigmoid_gate))
    grad_gate = (hidden_grad * up_pre.astype(jnp.float32) * silu_slope).astype(jnp.bfloat16)
    grad_up = (hidden_grad * gate_value * sigmoid_gate).astype(jnp.bfloat16)
    replicas = lax.axis_size("dp")
    tensors = lax.axis_size("tensor")
    tokens, hidden = grad_gate.shape
    token_total = tokens * replicas
    sub = tokens // tensors
    spread = lax.all_to_all(
        grad_gate.reshape(tensors, sub, hidden), "tensor", split_axis=0, concat_axis=0, tiled=False
    )
    rows = tensors * hidden // replicas
    parts = spread.reshape(tensors, sub, hidden // rows, rows).transpose(0, 2, 1, 3)
    parts = parts.reshape(replicas, sub, rows)
    mine = lax.all_to_all(parts, "dp", split_axis=0, concat_axis=0, tiled=False)
    row_block = lax.all_gather(mine, "tensor", axis=0, tiled=False)
    row_block = row_block.transpose(1, 0, 2, 3).reshape(token_total, rows)
    factor_tile = lax.dot_general(
        row_block,
        lax.all_gather(grad_gate, "dp", axis=0, tiled=True),
        (((0,), (0,)), ((), ())),
        preferred_element_type=jnp.float32,
    )
    factor = factor_tile / jnp.float32(token_total)
    return (factor, grad_up)


def solution(mesh):
    placed = (P("dp", None), P("tensor", None), P("dp", "tensor"), P("dp", "tensor"))
    return jax.shard_map(
        local,
        mesh=mesh,
        in_specs=placed,
        out_specs=(P("dp", "tensor"), P("dp", "tensor")),
        check_vma=False,
    )
```

```python
import functools

import jax
import jax.numpy as jnp
from jax import lax
from jax.experimental import pallas as pl
from jax.experimental.pallas import tpu as pltpu
from jax.sharding import PartitionSpec as P

MESH = pl.DeviceIdType.MESH
NX, NZ = 4, 4
DP, TN = 16, 8
PLANE = ((0, 2), (1, 2), (0, 1), (0, 3), (1, 1), (1, 3), (1, 0))
ARRIVE = ((1, 0), (0, 1), (0, 3), (1, 1), (1, 3), (0, 2), (1, 2))


def exchange_kernel(b_ref, out_ref, s1, rall, col, row_t, send, loc, r1, r2, colr, colp, rr):
    tokens, hidden = b_ref.shape
    sub = tokens // TN
    rows = hidden // 2
    half_tok = tokens // 2
    dp = lax.axis_index("dp")
    tn = lax.axis_index("tensor")
    x, yh, c = lax.div(dp, 4), lax.rem(lax.div(dp, 2), 2), lax.rem(dp, 2)
    yl, z = lax.div(tn, NZ), lax.rem(tn, NZ)

    def dp_of(xi, yi, ci):
        return xi * 4 + yi * 2 + ci

    def tn_of(dy, dz):
        return lax.rem(yl + dy, 2) * NZ + lax.rem(z + dz, NZ)

    x1, x3, x2 = lax.rem(x + 1, NX), lax.rem(x + 3, NX), lax.rem(x + 2, NX)
    oy = 1 - yh
    xp, xm = dp_of(x1, yh, c), dp_of(x3, yh, c)
    yc, peer = dp_of(x, oy, c), dp_of(x, yh, 1 - c)
    zp, zm, yn = tn_of(0, 1), tn_of(0, 3), tn_of(1, 0)

    barrier = pltpu.get_barrier_semaphore()
    for dy, dz in PLANE:
        pl.semaphore_signal(barrier, inc=1, device_id=(dp, tn_of(dy, dz)), device_id_type=MESH)
    for k in range(1, DP):
        pl.semaphore_signal(barrier, inc=1, device_id=(lax.rem(dp + k, DP), tn), device_id_type=MESH)
    pl.semaphore_wait(barrier, len(PLANE) + DP - 1)

    started = []

    def push(src, dst, sem, where):
        copy = pltpu.make_async_remote_copy(
            src_ref=src,
            dst_ref=dst,
            send_sem=send.at[len(started)],
            recv_sem=sem,
            device_id=where,
            device_id_type=MESH,
        )
        copy.start()
        started.append(copy)

    def arrived(ref, sem):
        pltpu.make_async_copy(ref, ref, sem).wait()

    def tok(h):
        return pl.ds(h * half_tok, half_tok)

    def col_push(slot, h, where):
        push(col.at[slot, tok(h)], col.at[slot, tok(h)], colr.at[slot, h], (where, tn))

    def col_wait(slot, h):
        arrived(col.at[slot, tok(h)], colr.at[slot, h])

    def to_peer(slot):
        push(col.at[slot], col.at[slot], colp.at[lax.div(slot, 2)], (peer, tn))

    def seg(g):
        return pl.ds(g * (DP // 2), DP // 2)

    def row_push(p, g, where):
        push(rall.at[p, seg(g)], rall.at[p, seg(g)], rr.at[p, g], (dp, where))

    def row_wait(p, g):
        arrived(rall.at[p, seg(g)], rr.at[p, g])

    for dy, dz in PLANE:
        p = tn_of(dy, dz)
        push(b_ref.at[pl.ds(pl.multiple_of(p * sub, sub), sub)], s1.at[tn], r1.at[tn], (dp, p))
    own = pltpu.make_async_copy(b_ref, col.at[dp], loc.at[0])
    own.start()
    keep = pltpu.make_async_copy(
        b_ref.at[pl.ds(pl.multiple_of(tn * sub, sub), sub)], s1.at[tn], loc.at[1]
    )
    keep.start()

    def own_push(h, where):
        push(b_ref.at[tok(h)], col.at[dp, tok(h)], colr.at[dp, h], (where, tn))

    own_push(0, xp)
    own_push(1, xm)
    own_push(0, yc)
    own_push(1, yc)
    push(b_ref, col.at[dp], colp.at[lax.div(dp, 2)], (peer, tn))

    for n, (dy, dz) in enumerate(((0, 0),) + ARRIVE):
        t = tn_of(dy, dz)
        if n == 0:
            keep.wait()
        else:
            arrived(s1.at[t], r1.at[t])
        for h in range(2):
            owner = 2 * t + h
            src = s1.at[t, :, pl.ds(h * rows, rows)]
            dst = rall.at[tn, dp]
            remote = pltpu.make_async_remote_copy(
                src_ref=src,
                dst_ref=dst,
                send_sem=send.at[len(started)],
                recv_sem=r2.at[dp],
                device_id=(owner, tn),
                device_id_type=MESH,
            )
            local = pltpu.make_async_copy(src, dst, r2.at[dp])

            @pl.when(owner != dp)
            def _():
                remote.start()

            @pl.when(owner == dp)
            def _():
                local.start()

            started.append((remote, owner))

    own_push(1, xp)
    own_push(0, xm)

    a, b = dp_of(x3, yh, c), dp_of(x1, yh, c)
    col_wait(a, 0)
    col_push(a, 0, xp)
    col_wait(b, 1)
    col_push(b, 1, xm)

    for s in range(DP):
        arrived(rall.at[tn, s], r2.at[s])
    row_push(tn, 0, zp)
    row_push(tn, 1, zm)
    row_push(tn, 0, yn)
    row_push(tn, 1, yn)
    row_push(tn, 1, zp)
    row_push(tn, 0, zm)

    col_wait(yc, 0)
    col_wait(yc, 1)
    col_push(yc, 0, xp)
    col_push(yc, 1, xm)
    col_push(yc, 1, xp)
    col_push(yc, 0, xm)
    to_peer(yc)
    col_wait(a, 1)
    to_peer(a)
    col_wait(b, 0)
    to_peer(b)
    opp = dp_of(x2, yh, c)
    col_wait(opp, 0)
    col_wait(opp, 1)
    to_peer(opp)

    row_wait(zm, 0)
    row_push(zm, 0, zp)
    row_wait(zp, 1)
    row_push(zp, 1, zm)
    row_wait(yn, 0)
    row_wait(yn, 1)
    row_push(yn, 0, zp)
    row_push(yn, 1, zm)
    row_push(yn, 1, zp)
    row_push(yn, 0, zm)

    ca, cb = dp_of(x3, oy, c), dp_of(x1, oy, c)
    col_wait(ca, 0)
    col_push(ca, 0, xp)
    col_wait(cb, 1)
    col_push(cb, 1, xm)
    col_wait(ca, 1)
    to_peer(ca)
    col_wait(cb, 0)
    to_peer(cb)
    copp = dp_of(x2, oy, c)
    col_wait(copp, 0)
    col_wait(copp, 1)
    to_peer(copp)

    yzp, yzm, zo, yzo = tn_of(1, 1), tn_of(1, 3), tn_of(0, 2), tn_of(1, 2)
    own.wait()
    for k in range(DP // 2):
        slot = 2 * k + (1 - c)
        arrived(col.at[slot], colp.at[k])

    scale = 1.0 / (DP * tokens)

    def multiply(p, first):
        row_t[...] = rall[p].reshape(DP * sub, rows).T
        start = pl.multiple_of(p * sub, sub)

        @pl.loop(0, hidden // 256)
        def _(n):
            cols = pl.ds(pl.multiple_of(n * 256, 256), 256)
            rhs = col[:, pl.ds(start, sub), cols].reshape(DP * sub, 256)
            part = jnp.dot(row_t[...], rhs, preferred_element_type=jnp.float32) * scale
            if first:
                out_ref[:, cols] = part
            else:
                out_ref[:, cols] += part

    multiply(tn, True)
    row_wait(yzm, 0)
    row_push(yzm, 0, zp)
    row_wait(yzp, 1)
    row_push(yzp, 1, zm)
    row_wait(zp, 0)
    multiply(zp, False)
    row_wait(zm, 1)
    multiply(zm, False)
    multiply(yn, False)
    row_wait(zo, 0)
    row_wait(zo, 1)
    multiply(zo, False)
    row_wait(yzp, 0)
    multiply(yzp, False)
    row_wait(yzm, 1)
    multiply(yzm, False)
    row_wait(yzo, 0)
    row_wait(yzo, 1)
    multiply(yzo, False)

    for item in started:
        if isinstance(item, tuple):
            remote, owner = item

            @pl.when(owner != dp)
            def _():
                remote.wait_send()
        else:
            item.wait_send()


def exchange(grad_gate):
    tokens, hidden = grad_gate.shape
    sub, rows = tokens // TN, hidden // 2
    return pl.pallas_call(
        exchange_kernel,
        out_shape=jax.ShapeDtypeStruct((rows, hidden), jnp.float32),
        in_specs=[pl.BlockSpec(memory_space=pltpu.VMEM)],
        out_specs=pl.BlockSpec(memory_space=pltpu.VMEM),
        scratch_shapes=[
            pltpu.VMEM((TN, sub, hidden), jnp.bfloat16),
            pltpu.VMEM((TN, DP, sub, rows), jnp.bfloat16),
            pltpu.VMEM((DP, tokens, hidden), jnp.bfloat16),
            pltpu.VMEM((rows, DP * sub), jnp.bfloat16),
            pltpu.SemaphoreType.DMA((64,)),
            pltpu.SemaphoreType.DMA((2,)),
            pltpu.SemaphoreType.DMA((TN,)),
            pltpu.SemaphoreType.DMA((DP,)),
            pltpu.SemaphoreType.DMA((DP, 2)),
            pltpu.SemaphoreType.DMA((DP // 2,)),
            pltpu.SemaphoreType.DMA((TN, 2)),
        ],
        compiler_params=pltpu.CompilerParams(
            collective_id=0, has_side_effects=True, vmem_limit_bytes=58 * 1024 * 1024
        ),
        name="exchange",
    )(grad_gate)


def local(grad_out, down_weight, gate_pre, up_pre):
    hidden_grad = lax.dot_general(
        grad_out, down_weight, (((1,), (1,)), ((), ())), preferred_element_type=jnp.float32
    )
    gate_value = gate_pre.astype(jnp.float32)
    sigmoid_gate = jax.nn.sigmoid(gate_value)
    silu_slope = sigmoid_gate * (1.0 + gate_value * (1.0 - sigmoid_gate))
    grad_gate = (hidden_grad * up_pre.astype(jnp.float32) * silu_slope).astype(jnp.bfloat16)
    grad_up = (hidden_grad * gate_value * sigmoid_gate).astype(jnp.bfloat16)
    factor = exchange(grad_gate)
    return (factor, grad_up)


def solution(mesh):
    placed = (P("dp", None), P("tensor", None), P("dp", "tensor"), P("dp", "tensor"))
    return jax.shard_map(
        local,
        mesh=mesh,
        in_specs=placed,
        out_specs=(P("dp", "tensor"), P("dp", "tensor")),
        check_vma=False,
    )
```

```python
import jax
import jax.numpy as jnp
from jax import lax
from jax.experimental import pallas as pl
from jax.experimental.pallas import tpu as pltpu
from jax.sharding import PartitionSpec as P

MESH = pl.DeviceIdType.MESH
NX, NZ = 4, 4
DP, TN = 16, 8
CHUNK = 256
PLANE = ((0, 2), (1, 2), (0, 1), (0, 3), (1, 1), (1, 3), (1, 0))
ARRIVE = ((1, 0), (0, 1), (0, 3), (1, 1), (1, 3), (0, 2), (1, 2))
XORDER = (0, 1, 3, 2)


def factor_kernel(
    go_hbm, w_hbm, gate_hbm, up_hbm, out_ref, gu_ref,
    go, wv, gate, up, s1, rall, col,
    lin, send, r1, r2, colr, colp, rr,
):
    tokens, hidden = gu_ref.shape
    sub = tokens // TN
    rows = hidden // 2
    half_tok = tokens // 2
    chunks = hidden // CHUNK
    width = DP * sub
    dp = lax.axis_index("dp")
    tn = lax.axis_index("tensor")
    x, yh, c = lax.div(dp, 4), lax.rem(lax.div(dp, 2), 2), lax.rem(dp, 2)
    yl, z = lax.div(tn, NZ), lax.rem(tn, NZ)

    def dp_of(dx, yi, ci):
        return lax.rem(x + dx, NX) * 4 + yi * 2 + ci

    def tn_of(dy, dz):
        return lax.rem(yl + dy, 2) * NZ + lax.rem(z + dz, NZ)

    oy = 1 - yh
    xp, xm = dp_of(1, yh, c), dp_of(3, yh, c)
    yc, peer = dp_of(0, oy, c), dp_of(0, yh, 1 - c)
    zp, zm, yn = tn_of(0, 1), tn_of(0, 3), tn_of(1, 0)

    loads = [pltpu.make_async_copy(go_hbm, go, lin.at[chunks])]
    loads.append(pltpu.make_async_copy(gate_hbm, gate, lin.at[chunks + 1]))
    loads.append(pltpu.make_async_copy(up_hbm, up, lin.at[chunks + 2]))

    def w_load(n):
        rng = pl.ds(pl.multiple_of(n * CHUNK, CHUNK), CHUNK)
        return pltpu.make_async_copy(w_hbm.at[rng], wv.at[rng], lin.at[n])

    loads[0].start()
    w_load(0).start()
    loads[1].start()
    loads[2].start()
    for n in range(1, chunks):
        w_load(n).start()

    barrier = pltpu.get_barrier_semaphore()
    for dy, dz in PLANE:
        pl.semaphore_signal(barrier, inc=1, device_id=(dp, tn_of(dy, dz)), device_id_type=MESH)
    for k in range(1, DP):
        pl.semaphore_signal(barrier, inc=1, device_id=(lax.rem(dp + k, DP), tn), device_id_type=MESH)

    started = []

    def push(src, dst, sem, where):
        copy = pltpu.make_async_remote_copy(
            src_ref=src,
            dst_ref=dst,
            send_sem=send.at[len(started)],
            recv_sem=sem,
            device_id=where,
            device_id_type=MESH,
        )
        copy.start()
        started.append(copy)

    def arrived(ref, sem):
        pltpu.make_async_copy(ref, ref, sem).wait()

    def quarter(slot, h, k):
        return col.at[slot, pl.ds(k * half_tok, half_tok), pl.ds(h * rows, rows)]

    def col_push(slot, h, k, where):
        ref = quarter(slot, h, k)
        push(ref, ref, colr.at[slot, 2 * h + k], (where, tn))

    def col_wait(slot, h, k):
        arrived(quarter(slot, h, k), colr.at[slot, 2 * h + k])

    def to_peer(slot):
        push(col.at[slot], col.at[slot], colp.at[lax.div(slot, 2)], (peer, tn))

    def from_peer(slot):
        arrived(col.at[slot], colp.at[lax.div(slot, 2)])

    def seg(p, i):
        return rall.at[p, pl.ds(lax.rem(x + XORDER[i], NX) * 4, 4)]

    def row_push(p, i, where):
        push(seg(p, i), seg(p, i), rr.at[p, i], (dp, where))

    def row_wait(p, i):
        arrived(seg(p, i), rr.at[p, i])

    def slice_of(p, h):
        return col.at[dp, pl.ds(pl.multiple_of(p * sub, sub), sub), pl.ds(h * rows, rows)]

    def scatter_plane(h):
        for dy, dz in PLANE:
            p = tn_of(dy, dz)
            push(slice_of(p, h), s1.at[h, tn], r1.at[h, tn], (dp, p))

    def scatter_rows(h):
        for n, (dy, dz) in enumerate(((0, 0),) + ARRIVE):
            t = tn_of(dy, dz)
            if n == 0:
                src = slice_of(tn, h)
            else:
                arrived(s1.at[h, t], r1.at[h, t])
                src = s1.at[h, t]
            owner = 2 * t + h
            dst = rall.at[tn, dp]
            remote = pltpu.make_async_remote_copy(
                src_ref=src,
                dst_ref=dst,
                send_sem=send.at[len(started)],
                recv_sem=r2.at[dp],
                device_id=(owner, tn),
                device_id_type=MESH,
            )
            local = pltpu.make_async_copy(src, dst, r2.at[dp])

            @pl.when(owner != dp)
            def _():
                remote.start()

            @pl.when(owner == dp)
            def _():
                local.start()

            started.append((remote, owner))

    def chunk(n):
        w_load(n).wait()
        cols = pl.ds(pl.multiple_of(n * CHUNK, CHUNK), CHUNK)
        grad = lax.dot_general(
            go[...], wv[cols, :], (((1,), (1,)), ((), ())), preferred_element_type=jnp.float32
        )
        g = gate[:, cols].astype(jnp.float32)
        s = 1.0 / (1.0 + jnp.exp(-g))
        gu_ref[:, cols] = (grad * g * s).astype(jnp.bfloat16)
        slope = s * (1.0 + g * (1.0 - s))
        col[dp, :, cols] = (grad * up[:, cols].astype(jnp.float32) * slope).astype(jnp.bfloat16)

    for load in loads:
        load.wait()
    first_half = -(-rows // CHUNK) + 1

    @pl.loop(0, first_half)
    def _(n):
        chunk(n)

    pl.semaphore_wait(barrier, len(PLANE) + DP - 1)
    scatter_plane(0)
    col_push(dp, 0, 0, xp)
    col_push(dp, 0, 1, xm)

    @pl.loop(first_half, chunks)
    def _(n):
        chunk(n)

    col_push(dp, 0, 0, yc)
    col_push(dp, 0, 1, yc)
    scatter_plane(1)
    to_peer(dp)

    scatter_rows(0)
    col_push(dp, 0, 1, xp)
    col_push(dp, 0, 0, xm)
    scatter_rows(1)
    for k in (0, 1):
        col_push(dp, 1, k, xp)
        col_push(dp, 1, 1 - k, xm)

    a, b, opp = dp_of(3, yh, c), dp_of(1, yh, c), dp_of(2, yh, c)
    ca, cb, copp = dp_of(3, oy, c), dp_of(1, oy, c), dp_of(2, oy, c)

    def x_relay(left, right, h):
        col_wait(left, h, 0)
        col_push(left, h, 0, xp)
        col_wait(right, h, 1)
        col_push(right, h, 1, xm)

    x_relay(a, b, 0)

    for i, dx in enumerate(XORDER):
        for yi in range(2):
            for ci in range(2):
                s = lax.rem(x + dx, NX) * 4 + yi * 2 + ci
                arrived(rall.at[tn, s], r2.at[s])
        row_push(tn, i, zp)
        row_push(tn, i, zm)
        row_push(tn, i, yn)
    col_push(dp, 1, 0, yc)
    col_push(dp, 1, 1, yc)

    x_relay(a, b, 1)

    def cross(h):
        for k in range(2):
            col_wait(yc, h, k)
        for k in range(2):
            col_push(yc, h, k, xp)
            col_push(yc, h, 1 - k, xm)

    cross(0)

    def z_relay(left, right, i):
        if i % 2 == 0:
            row_wait(left, i)
            row_push(left, i, zp)
        else:
            row_wait(right, i)
            row_push(right, i, zm)

    for i in range(4):
        z_relay(zm, zp, i)

    def from_y(i):
        row_wait(yn, i)
        row_push(yn, i, zp)
        row_push(yn, i, zm)

    from_y(0)
    from_y(1)
    cross(1)
    to_peer(yc)

    def complete(slot, done):
        for h in range(2):
            for k in range(2):
                if (h, k) not in done:
                    col_wait(slot, h, k)
        to_peer(slot)

    plus, minus = ((0, 0), (1, 0)), ((0, 1), (1, 1))
    complete(a, plus)
    complete(b, minus)
    complete(opp, ())

    order = [dp_of(dx, yh, ci) for dx in (0, 3, 1, 2) for ci in range(2)]
    order += [dp_of(dx, oy, ci) for dx in (0, 3, 1, 2) for ci in range(2)]
    near, mid, far = (0, 8), (8, 12), (12, 16)
    scale = 1.0 / (DP * tokens)

    def turn(p):
        @pl.loop(0, rows // 128)
        def _(m):
            lanes = pl.ds(pl.multiple_of(m * 128, 128), 128)
            tile = jnp.concatenate([rall[p, s, :, lanes] for s in order], axis=0)
            wv[lanes, pl.ds(pl.multiple_of(p * width, width), width)] = tile.T

    def multiply(ps, span, first=False):
        lo, hi = span
        k = (hi - lo) * sub

        @pl.loop(0, hidden // 256)
        def _(n):
            cols = pl.ds(pl.multiple_of(n * 256, 256), 256)
            lhs = [
                wv[0:rows, pl.ds(pl.multiple_of(p * width + lo * sub, 128), k)] for p in ps
            ]
            rhs = [
                col[s, pl.ds(pl.multiple_of(p * sub, sub), sub), cols]
                for p in ps
                for s in order[lo:hi]
            ]
            part = scale * jnp.dot(
                jnp.concatenate(lhs, axis=1),
                jnp.concatenate(rhs, axis=0),
                preferred_element_type=jnp.float32,
            )
            if first:
                out_ref[:, cols] = part
            else:
                out_ref[:, cols] += part

    yzp, yzm, zo, yzo = tn_of(1, 1), tn_of(1, 3), tn_of(0, 2), tn_of(1, 2)

    turn(tn)
    row_wait(zp, 0)
    row_wait(zp, 2)
    turn(zp)
    for slot in (dp_of(0, yh, 1 - c), dp_of(3, yh, 1 - c), dp_of(1, yh, 1 - c), dp_of(2, yh, 1 - c)):
        from_peer(slot)
    multiply((tn, zp), near, True)
    from_y(2)
    x_relay(ca, cb, 0)
    z_relay(yzm, yzp, 0)
    z_relay(yzm, yzp, 1)
    row_wait(zm, 1)
    row_wait(zm, 3)
    turn(zm)
    from_y(3)
    for i in range(4):
        row_wait(zo, i)
    turn(zo)
    multiply((zm, zo), near)
    x_relay(ca, cb, 1)
    z_relay(yzm, yzp, 2)
    z_relay(yzm, yzp, 3)
    turn(yn)
    complete(ca, plus)
    from_peer(dp_of(0, oy, 1 - c))
    from_peer(dp_of(3, oy, 1 - c))
    multiply((tn, zp, zm, zo), mid)
    row_wait(yzp, 0)
    row_wait(yzp, 2)
    turn(yzp)
    multiply((yn, yzp), near)
    complete(cb, minus)
    complete(copp, ())
    row_wait(yzm, 1)
    row_wait(yzm, 3)
    turn(yzm)
    from_peer(dp_of(1, oy, 1 - c))
    from_peer(dp_of(2, oy, 1 - c))
    multiply((tn, zp, zm, zo), far)
    for i in range(4):
        row_wait(yzo, i)
    turn(yzo)
    multiply((yzm, yzo), near)
    multiply((yn, yzp, yzm, yzo), mid)
    multiply((yn, yzp, yzm, yzo), far)

    for item in started:
        if isinstance(item, tuple):
            remote, owner = item

            @pl.when(owner != dp)
            def _():
                remote.wait_send()
        else:
            item.wait_send()


def local(grad_out, down_weight, gate_pre, up_pre):
    tokens, hidden = gate_pre.shape
    depth = grad_out.shape[1]
    sub, rows = tokens // TN, hidden // 2
    return tuple(
        pl.pallas_call(
            factor_kernel,
            out_shape=(
                pltpu.VMEM((rows, hidden), jnp.float32),
                pltpu.VMEM((tokens, hidden), jnp.bfloat16),
            ),
            in_specs=[pl.BlockSpec(memory_space=pl.ANY)] * 4,
            out_specs=(
                pl.BlockSpec(memory_space=pltpu.VMEM),
                pl.BlockSpec(memory_space=pltpu.VMEM),
            ),
            scratch_shapes=[
                pltpu.VMEM((tokens, depth), jnp.bfloat16),
                pltpu.VMEM((hidden, depth), jnp.bfloat16),
                pltpu.VMEM((tokens, hidden), jnp.bfloat16),
                pltpu.VMEM((tokens, hidden), jnp.bfloat16),
                pltpu.VMEM((2, TN, sub, rows), jnp.bfloat16),
                pltpu.VMEM((TN, DP, sub, rows), jnp.bfloat16),
                pltpu.VMEM((DP, tokens, hidden), jnp.bfloat16),
                pltpu.SemaphoreType.DMA((hidden // CHUNK + 3,)),
                pltpu.SemaphoreType.DMA((128,)),
                pltpu.SemaphoreType.DMA((2, TN)),
                pltpu.SemaphoreType.DMA((DP,)),
                pltpu.SemaphoreType.DMA((DP, 4)),
                pltpu.SemaphoreType.DMA((DP // 2,)),
                pltpu.SemaphoreType.DMA((TN, 4)),
            ],
            compiler_params=pltpu.CompilerParams(
                collective_id=0, has_side_effects=True, vmem_limit_bytes=52 * 1024 * 1024
            ),
            name="factor",
        )(grad_out, down_weight, gate_pre, up_pre)
    )


def solution(mesh):
    placed = (P("dp", None), P("tensor", None), P("dp", "tensor"), P("dp", "tensor"))
    return jax.shard_map(
        local,
        mesh=mesh,
        in_specs=placed,
        out_specs=(P("dp", "tensor"), P("dp", "tensor")),
        check_vma=False,
    )
```

```python
import jax
import jax.numpy as jnp
from jax import lax
from jax.experimental import pallas as pl
from jax.experimental.pallas import tpu as pltpu
from jax.sharding import PartitionSpec as P

MESH = pl.DeviceIdType.MESH
NX, NZ = 4, 4
DP, TN = 16, 8
CHUNK = 256
NTILE = 1792
PLANE = ((0, 2), (1, 2), (0, 1), (0, 3), (1, 1), (1, 3), (1, 0))
XORDER = (0, 1, 3, 2)


def factor_kernel(
    go_hbm, w_hbm, gate_hbm, up_hbm, out_ref, gu_ref,
    go, wv, gate, up, s1, rall, col,
    lin, send, r1, r2, colr, colp, rr,
):
    tokens, hidden = gu_ref.shape
    sub = tokens // TN
    rows = hidden // 2
    half_tok = tokens // 2
    chunks = hidden // CHUNK
    width = DP * sub
    dp = lax.axis_index("dp")
    tn = lax.axis_index("tensor")
    x, yh, c = lax.div(dp, 4), lax.rem(lax.div(dp, 2), 2), lax.rem(dp, 2)
    yl, z = lax.div(tn, NZ), lax.rem(tn, NZ)

    def dp_of(dx, yi, ci):
        return lax.rem(x + dx, NX) * 4 + yi * 2 + ci

    def tn_of(dy, dz):
        return lax.rem(yl + dy, 2) * NZ + lax.rem(z + dz, NZ)

    oy = 1 - yh
    xp, xm = dp_of(1, yh, c), dp_of(3, yh, c)
    yc, peer = dp_of(0, oy, c), dp_of(0, yh, 1 - c)
    zp, zm, yn = tn_of(0, 1), tn_of(0, 3), tn_of(1, 0)

    loads = [pltpu.make_async_copy(go_hbm, go, lin.at[chunks])]
    loads.append(pltpu.make_async_copy(gate_hbm, gate, lin.at[chunks + 1]))
    loads.append(pltpu.make_async_copy(up_hbm, up, lin.at[chunks + 2]))

    def w_load(n):
        rng = pl.ds(pl.multiple_of(n * CHUNK, CHUNK), CHUNK)
        return pltpu.make_async_copy(w_hbm.at[rng], wv.at[rng], lin.at[n])

    loads[0].start()
    w_load(0).start()
    loads[1].start()
    loads[2].start()
    for n in range(1, chunks):
        w_load(n).start()

    barrier = pltpu.get_barrier_semaphore()
    for dy, dz in PLANE:
        pl.semaphore_signal(barrier, inc=1, device_id=(dp, tn_of(dy, dz)), device_id_type=MESH)
    for k in range(1, DP):
        pl.semaphore_signal(barrier, inc=1, device_id=(lax.rem(dp + k, DP), tn), device_id_type=MESH)

    started = []

    def push(src, dst, sem, where):
        copy = pltpu.make_async_remote_copy(
            src_ref=src,
            dst_ref=dst,
            send_sem=send.at[len(started)],
            recv_sem=sem,
            device_id=where,
            device_id_type=MESH,
        )
        copy.start()
        started.append(copy)

    def arrived(ref, sem):
        pltpu.make_async_copy(ref, ref, sem).wait()

    def quarter(slot, h, k):
        return col.at[slot, pl.ds(k * half_tok, half_tok), pl.ds(h * rows, rows)]

    def col_push(slot, h, k, where):
        ref = quarter(slot, h, k)
        push(ref, ref, colr.at[slot, 2 * h + k], (where, tn))

    def col_wait(slot, h, k):
        arrived(quarter(slot, h, k), colr.at[slot, 2 * h + k])

    def to_peer(slot):
        push(col.at[slot], col.at[slot], colp.at[lax.div(slot, 2)], (peer, tn))

    def from_peer(slot):
        arrived(col.at[slot], colp.at[lax.div(slot, 2)])

    def seg(p, i):
        return rall.at[p, pl.ds(lax.rem(x + XORDER[i], NX) * 4, 4)]

    def row_push(p, i, where):
        push(seg(p, i), seg(p, i), rr.at[p, i], (dp, where))

    def row_wait(p, i):
        arrived(seg(p, i), rr.at[p, i])

    def slice_of(p, h):
        return col.at[dp, pl.ds(pl.multiple_of(p * sub, sub), sub), pl.ds(h * rows, rows)]

    def scatter_plane(h):
        for dy, dz in PLANE:
            p = tn_of(dy, dz)
            push(slice_of(p, h), s1.at[h, tn], r1.at[h, tn], (dp, p))
        pltpu.make_async_copy(slice_of(tn, h), s1.at[h, tn], r1.at[h, tn]).start()

    def scatter_rows(h):
        for dx in XORDER:
            for yb in range(2):
                t = lax.rem(x + dx, NX) * 2 + yb
                arrived(s1.at[h, t], r1.at[h, t])
                owner = 2 * t + h
                src, dst = s1.at[h, t], rall.at[tn, dp]
                remote = pltpu.make_async_remote_copy(
                    src_ref=src,
                    dst_ref=dst,
                    send_sem=send.at[len(started)],
                    recv_sem=r2.at[dp],
                    device_id=(owner, tn),
                    device_id_type=MESH,
                )
                local = pltpu.make_async_copy(src, dst, r2.at[dp])

                @pl.when(owner != dp)
                def _():
                    remote.start()

                @pl.when(owner == dp)
                def _():
                    local.start()

                started.append((remote, owner))

    def chunk(n):
        w_load(n).wait()
        cols = pl.ds(pl.multiple_of(n * CHUNK, CHUNK), CHUNK)
        grad = lax.dot_general(
            go[...], wv[cols, :], (((1,), (1,)), ((), ())), preferred_element_type=jnp.float32
        )
        g = gate[:, cols].astype(jnp.float32)
        s = 1.0 / (1.0 + jnp.exp(-g))
        gu_ref[:, cols] = (grad * g * s).astype(jnp.bfloat16)
        slope = s * (1.0 + g * (1.0 - s))
        col[dp, :, cols] = (grad * up[:, cols].astype(jnp.float32) * slope).astype(jnp.bfloat16)

    for load in loads:
        load.wait()
    first_half = -(-rows // CHUNK) + 1

    @pl.loop(0, first_half)
    def _(n):
        chunk(n)

    a, b, opp = dp_of(3, yh, c), dp_of(1, yh, c), dp_of(2, yh, c)
    ca, cb, copp = dp_of(3, oy, c), dp_of(1, oy, c), dp_of(2, oy, c)
    yzp, yzm, zo, yzo = tn_of(1, 1), tn_of(1, 3), tn_of(0, 2), tn_of(1, 2)

    def x_relay(left, right, h):
        col_wait(left, h, 0)
        col_push(left, h, 0, xp)
        col_wait(right, h, 1)
        col_push(right, h, 1, xm)

    def gather_rows(i):
        xs = lax.rem(x + XORDER[i], NX) * 4
        for k in range(4):
            arrived(rall.at[tn, xs + k], r2.at[xs + k])
        row_push(tn, i, zp)
        row_push(tn, i, zm)

    def own_ring(h):
        for k in (0, 1):
            col_push(dp, h, k, xp)
            col_push(dp, h, 1 - k, xm)

    def to_cross(h):
        col_push(dp, h, 0, yc)
        col_push(dp, h, 1, yc)

    def cross(h):
        for k in range(2):
            col_wait(yc, h, k)
        for k in range(2):
            col_push(yc, h, k, xp)
            col_push(yc, h, 1 - k, xm)

    def z_relay(left, right, i):
        if i % 2 == 0:
            row_wait(left, i)
            row_push(left, i, zp)
        else:
            row_wait(right, i)
            row_push(right, i, zm)

    def from_y(i):
        row_wait(yn, i)
        row_push(yn, i, zp)
        row_push(yn, i, zm)

    def rest(p, segments):
        for i in segments:
            row_wait(p, i)

    def complete(slot, done):
        for h in range(2):
            for k in range(2):
                if (h, k) not in done:
                    col_wait(slot, h, k)
        to_peer(slot)

    plus, minus = ((0, 0), (1, 0)), ((0, 1), (1, 1))

    order = [dp_of(dx, yh, ci) for dx in (0, 3, 1, 2) for ci in range(2)]
    order += [dp_of(dx, oy, ci) for dx in (0, 3, 1, 2) for ci in range(2)]
    near, mid, far = (0, 8), (8, 12), (12, 16)
    scale = 1.0 / (DP * tokens)

    def peer_side(*dxs, yi):
        for dx in dxs:
            from_peer(dp_of(dx, yi, 1 - c))

    def turn(p):
        @pl.loop(0, rows // 128)
        def _(m):
            lanes = pl.ds(pl.multiple_of(m * 128, 128), 128)
            tile = jnp.concatenate([rall[p, s, :, lanes] for s in order], axis=0)
            wv[lanes, pl.ds(pl.multiple_of(p * width, width), width)] = tile.T

    def multiply(ps, span, first=False):
        lo, hi = span
        k = (hi - lo) * sub

        @pl.loop(0, hidden // NTILE)
        def _(n):
            cols = pl.ds(pl.multiple_of(n * NTILE, NTILE), NTILE)
            lhs = [
                wv[0:rows, pl.ds(pl.multiple_of(p * width + lo * sub, 128), k)] for p in ps
            ]
            rhs = [
                col[s, pl.ds(pl.multiple_of(p * sub, sub), sub), cols]
                for p in ps
                for s in order[lo:hi]
            ]
            part = scale * jnp.dot(
                jnp.concatenate(lhs, axis=1),
                jnp.concatenate(rhs, axis=0),
                preferred_element_type=jnp.float32,
            )
            if first:
                out_ref[:, cols] = part
            else:
                out_ref[:, cols] += part

    pl.semaphore_wait(barrier, len(PLANE) + DP - 1)
    scatter_plane(0)
    col_push(dp, 0, 0, xp)
    col_push(dp, 0, 1, xm)

    @pl.loop(first_half, chunks)
    def _(n):
        chunk(n)

    scatter_plane(1)
    to_peer(dp)
    scatter_rows(0)
    col_push(dp, 0, 1, xp)
    col_push(dp, 0, 0, xm)
    scatter_rows(1)
    own_ring(1)
    to_cross(0)
    x_relay(a, b, 0)
    gather_rows(0)
    row_push(tn, 0, yn)
    to_cross(1)
    gather_rows(1)
    gather_rows(2)
    gather_rows(3)
    row_push(tn, 1, yn)
    row_push(tn, 2, yn)
    row_push(tn, 3, yn)
    turn(tn)
    z_relay(zm, zp, 0)
    z_relay(zm, zp, 1)
    x_relay(a, b, 1)
    z_relay(zm, zp, 2)
    cross(0)
    z_relay(zm, zp, 3)
    complete(a, plus)
    complete(b, minus)
    rest(zp, (0, 2))
    rest(zm, (1, 3))
    turn(zp)
    turn(zm)
    from_y(0)
    complete(opp, ())
    peer_side(0, 1, 2, 3, yi=yh)
    multiply((tn, zp), near, True)
    rest(zo, range(4))
    turn(zo)
    cross(1)
    to_peer(yc)
    multiply((zm, zo), near)
    from_y(1)
    x_relay(ca, cb, 0)
    z_relay(yzm, yzp, 0)
    from_y(2)
    z_relay(yzm, yzp, 1)
    from_y(3)
    turn(yn)
    x_relay(ca, cb, 1)
    complete(ca, plus)
    complete(cb, minus)
    multiply((yn,), near)
    peer_side(0, 3, yi=oy)
    z_relay(yzm, yzp, 2)
    multiply((tn, zp, zm, zo), mid)
    multiply((yn,), mid)
    z_relay(yzm, yzp, 3)
    complete(copp, ())
    rest(yzp, (0, 2))
    rest(yzm, (1, 3))
    turn(yzp)
    turn(yzm)
    multiply((yzp, yzm), near)
    peer_side(1, 2, yi=oy)
    multiply((tn, zp, zm, zo), far)
    multiply((yn, yzp, yzm), far)
    multiply((yzp, yzm), mid)
    rest(yzo, range(4))
    turn(yzo)
    multiply((yzo,), (0, 16))

    for item in started:
        if isinstance(item, tuple):
            remote, owner = item

            @pl.when(owner != dp)
            def _():
                remote.wait_send()
        else:
            item.wait_send()


def local(grad_out, down_weight, gate_pre, up_pre):
    tokens, hidden = gate_pre.shape
    depth = grad_out.shape[1]
    sub, rows = tokens // TN, hidden // 2
    return tuple(
        pl.pallas_call(
            factor_kernel,
            out_shape=(
                pltpu.VMEM((rows, hidden), jnp.float32),
                pltpu.VMEM((tokens, hidden), jnp.bfloat16),
            ),
            in_specs=[pl.BlockSpec(memory_space=pl.ANY)] * 4,
            out_specs=(
                pl.BlockSpec(memory_space=pltpu.VMEM),
                pl.BlockSpec(memory_space=pltpu.VMEM),
            ),
            scratch_shapes=[
                pltpu.VMEM((tokens, depth), jnp.bfloat16),
                pltpu.VMEM((hidden, depth), jnp.bfloat16),
                pltpu.VMEM((tokens, hidden), jnp.bfloat16),
                pltpu.VMEM((tokens, hidden), jnp.bfloat16),
                pltpu.VMEM((2, TN, sub, rows), jnp.bfloat16),
                pltpu.VMEM((TN, DP, sub, rows), jnp.bfloat16),
                pltpu.VMEM((DP, tokens, hidden), jnp.bfloat16),
                pltpu.SemaphoreType.DMA((hidden // CHUNK + 3,)),
                pltpu.SemaphoreType.DMA((128,)),
                pltpu.SemaphoreType.DMA((2, TN)),
                pltpu.SemaphoreType.DMA((DP,)),
                pltpu.SemaphoreType.DMA((DP, 4)),
                pltpu.SemaphoreType.DMA((DP // 2,)),
                pltpu.SemaphoreType.DMA((TN, 4)),
            ],
            compiler_params=pltpu.CompilerParams(
                collective_id=0, has_side_effects=True, vmem_limit_bytes=52 * 1024 * 1024
            ),
            name="factor",
        )(grad_out, down_weight, gate_pre, up_pre)
    )


def solution(mesh):
    placed = (P("dp", None), P("tensor", None), P("dp", "tensor"), P("dp", "tensor"))
    return jax.shard_map(
        local,
        mesh=mesh,
        in_specs=placed,
        out_specs=(P("dp", "tensor"), P("dp", "tensor")),
        check_vma=False,
    )
```

```python
import jax
import jax.numpy as jnp
from jax import lax
from jax.experimental import pallas as pl
from jax.experimental.pallas import tpu as pltpu
from jax.sharding import PartitionSpec as P

MESH = pl.DeviceIdType.MESH
NX, NZ = 4, 4
DP, TN = 16, 8
CHUNK = 256
NTILE = 1792
PLANE = ((0, 2), (1, 2), (0, 1), (0, 3), (1, 1), (1, 3), (1, 0))
XORDER = (0, 1, 3, 2)


def factor_kernel(
    go_hbm, w_hbm, gate_hbm, up_hbm, out_ref, gu_ref,
    go, wv, gate, up, s1, rall, col,
    lin, send, r1, r2, colr, colp, rr,
):
    tokens, hidden = gu_ref.shape
    sub = tokens // TN
    rows = hidden // 2
    half_tok = tokens // 2
    chunks = hidden // CHUNK
    width = DP * sub
    dp = lax.axis_index("dp")
    tn = lax.axis_index("tensor")
    x, yh, c = lax.div(dp, 4), lax.rem(lax.div(dp, 2), 2), lax.rem(dp, 2)
    yl, z = lax.div(tn, NZ), lax.rem(tn, NZ)

    def dp_of(dx, yi, ci):
        return lax.rem(x + dx, NX) * 4 + yi * 2 + ci

    def tn_of(dy, dz):
        return lax.rem(yl + dy, 2) * NZ + lax.rem(z + dz, NZ)

    oy = 1 - yh
    xp, xm = dp_of(1, yh, c), dp_of(3, yh, c)
    yc, peer = dp_of(0, oy, c), dp_of(0, yh, 1 - c)
    zp, zm, yn = tn_of(0, 1), tn_of(0, 3), tn_of(1, 0)

    loads = [pltpu.make_async_copy(go_hbm, go, lin.at[chunks])]
    loads.append(pltpu.make_async_copy(gate_hbm, gate, lin.at[chunks + 1]))
    loads.append(pltpu.make_async_copy(up_hbm, up, lin.at[chunks + 2]))

    def w_load(n):
        rng = pl.ds(pl.multiple_of(n * CHUNK, CHUNK), CHUNK)
        return pltpu.make_async_copy(w_hbm.at[rng], wv.at[rng], lin.at[n])

    loads[0].start()
    w_load(0).start()
    loads[1].start()
    loads[2].start()
    for n in range(1, chunks):
        w_load(n).start()

    barrier = pltpu.get_barrier_semaphore()
    for dy, dz in PLANE:
        pl.semaphore_signal(barrier, inc=1, device_id=(dp, tn_of(dy, dz)), device_id_type=MESH)
    for k in range(1, DP):
        pl.semaphore_signal(barrier, inc=1, device_id=(lax.rem(dp + k, DP), tn), device_id_type=MESH)

    started = []

    def push(src, dst, sem, where):
        copy = pltpu.make_async_remote_copy(
            src_ref=src,
            dst_ref=dst,
            send_sem=send.at[len(started)],
            recv_sem=sem,
            device_id=where,
            device_id_type=MESH,
        )
        copy.start()
        started.append(copy)

    def arrived(ref, sem):
        pltpu.make_async_copy(ref, ref, sem).wait()

    def quarter(slot, h, k):
        return col.at[slot, pl.ds(k * half_tok, half_tok), pl.ds(h * rows, rows)]

    def col_push(slot, h, k, where):
        ref = quarter(slot, h, k)
        push(ref, ref, colr.at[slot, 2 * h + k], (where, tn))

    def col_wait(slot, h, k):
        arrived(quarter(slot, h, k), colr.at[slot, 2 * h + k])

    def to_peer(slot):
        push(col.at[slot], col.at[slot], colp.at[lax.div(slot, 2)], (peer, tn))

    def from_peer(slot):
        arrived(col.at[slot], colp.at[lax.div(slot, 2)])

    def seg(p, i):
        return rall.at[p, pl.ds(lax.rem(x + XORDER[i], NX) * 4, 4)]

    def row_push(p, i, where):
        push(seg(p, i), seg(p, i), rr.at[p, i], (dp, where))

    def row_wait(p, i):
        arrived(seg(p, i), rr.at[p, i])

    def slice_of(p, h):
        return col.at[dp, pl.ds(pl.multiple_of(p * sub, sub), sub), pl.ds(h * rows, rows)]

    def scatter_plane(h):
        for dy, dz in PLANE:
            p = tn_of(dy, dz)
            push(slice_of(p, h), s1.at[h, tn], r1.at[h, tn], (dp, p))
        pltpu.make_async_copy(slice_of(tn, h), s1.at[h, tn], r1.at[h, tn]).start()

    def scatter_rows(h):
        for dx in XORDER:
            for yb in range(2):
                t = lax.rem(x + dx, NX) * 2 + yb
                arrived(s1.at[h, t], r1.at[h, t])
                owner = 2 * t + h
                src, dst = s1.at[h, t], rall.at[tn, dp]
                remote = pltpu.make_async_remote_copy(
                    src_ref=src,
                    dst_ref=dst,
                    send_sem=send.at[len(started)],
                    recv_sem=r2.at[dp],
                    device_id=(owner, tn),
                    device_id_type=MESH,
                )
                local = pltpu.make_async_copy(src, dst, r2.at[dp])

                @pl.when(owner != dp)
                def _():
                    remote.start()

                @pl.when(owner == dp)
                def _():
                    local.start()

                started.append((remote, owner))

    def chunk(n):
        w_load(n).wait()
        cols = pl.ds(pl.multiple_of(n * CHUNK, CHUNK), CHUNK)
        grad = lax.dot_general(
            go[...], wv[cols, :], (((1,), (1,)), ((), ())), preferred_element_type=jnp.float32
        )
        g = gate[:, cols].astype(jnp.float32)
        s = 1.0 / (1.0 + jnp.exp(-g))
        gu_ref[:, cols] = (grad * g * s).astype(jnp.bfloat16)
        slope = s * (1.0 + g * (1.0 - s))
        col[dp, :, cols] = (grad * up[:, cols].astype(jnp.float32) * slope).astype(jnp.bfloat16)

    for load in loads:
        load.wait()
    first_half = -(-rows // CHUNK) + 1

    @pl.loop(0, first_half)
    def _(n):
        chunk(n)

    a, b, opp = dp_of(3, yh, c), dp_of(1, yh, c), dp_of(2, yh, c)
    ca, cb, copp = dp_of(3, oy, c), dp_of(1, oy, c), dp_of(2, oy, c)
    yzp, yzm, zo, yzo = tn_of(1, 1), tn_of(1, 3), tn_of(0, 2), tn_of(1, 2)

    def x_relay(left, right, h):
        col_wait(left, h, 0)
        col_push(left, h, 0, xp)
        col_wait(right, h, 1)
        col_push(right, h, 1, xm)

    def gather_rows(i):
        xs = lax.rem(x + XORDER[i], NX) * 4
        for k in range(4):
            arrived(rall.at[tn, xs + k], r2.at[xs + k])
        row_push(tn, i, zp)
        row_push(tn, i, zm)

    def own_ring(h):
        for k in (0, 1):
            col_push(dp, h, k, xp)
            col_push(dp, h, 1 - k, xm)

    def to_cross(h):
        col_push(dp, h, 0, yc)
        col_push(dp, h, 1, yc)

    def cross(h):
        for k in range(2):
            col_wait(yc, h, k)
        for k in range(2):
            col_push(yc, h, k, xp)
            col_push(yc, h, 1 - k, xm)

    def z_relay(left, right, i):
        if i % 2 == 0:
            row_wait(left, i)
            row_push(left, i, zp)
        else:
            row_wait(right, i)
            row_push(right, i, zm)

    def from_y(i):
        row_wait(yn, i)
        row_push(yn, i, zp)
        row_push(yn, i, zm)

    def rest(p, segments):
        for i in segments:
            row_wait(p, i)

    def complete(slot, done):
        for h in range(2):
            for k in range(2):
                if (h, k) not in done:
                    col_wait(slot, h, k)
        to_peer(slot)

    plus, minus = ((0, 0), (1, 0)), ((0, 1), (1, 1))

    order = [dp_of(dx, yh, ci) for dx in (0, 3, 1, 2) for ci in range(2)]
    order += [dp_of(dx, oy, ci) for dx in (0, 3, 1, 2) for ci in range(2)]
    near, mid, far = (0, 8), (8, 12), (12, 16)
    scale = 1.0 / (DP * tokens)

    def peer_side(*dxs, yi):
        for dx in dxs:
            from_peer(dp_of(dx, yi, 1 - c))

    def turn(p):
        @pl.loop(0, rows // 128)
        def _(m):
            lanes = pl.ds(pl.multiple_of(m * 128, 128), 128)
            tile = jnp.concatenate([rall[p, s, :, lanes] for s in order], axis=0)
            wv[lanes, pl.ds(pl.multiple_of(p * width, width), width)] = tile.T

    def multiply(ps, span, first=False):
        lo, hi = span
        k = (hi - lo) * sub

        @pl.loop(0, hidden // NTILE)
        def _(n):
            cols = pl.ds(pl.multiple_of(n * NTILE, NTILE), NTILE)
            lhs = [
                wv[0:rows, pl.ds(pl.multiple_of(p * width + lo * sub, 128), k)] for p in ps
            ]
            rhs = [
                col[s, pl.ds(pl.multiple_of(p * sub, sub), sub), cols]
                for p in ps
                for s in order[lo:hi]
            ]
            part = scale * jnp.dot(
                jnp.concatenate(lhs, axis=1),
                jnp.concatenate(rhs, axis=0),
                preferred_element_type=jnp.float32,
            )
            if first:
                out_ref[:, cols] = part
            else:
                out_ref[:, cols] += part

    pl.semaphore_wait(barrier, len(PLANE) + DP - 1)
    scatter_plane(0)
    col_push(dp, 0, 0, xp)
    col_push(dp, 0, 1, xm)

    @pl.loop(first_half, chunks)
    def _(n):
        chunk(n)

    scatter_plane(1)
    to_peer(dp)
    scatter_rows(0)
    col_push(dp, 0, 1, xp)
    col_push(dp, 0, 0, xm)
    scatter_rows(1)
    own_ring(1)
    to_cross(0)
    x_relay(a, b, 0)
    gather_rows(0)
    row_push(tn, 0, yn)
    to_cross(1)
    gather_rows(1)
    gather_rows(2)
    gather_rows(3)
    row_push(tn, 1, yn)
    row_push(tn, 2, yn)
    row_push(tn, 3, yn)
    turn(tn)
    z_relay(zm, zp, 0)
    z_relay(zm, zp, 1)
    x_relay(a, b, 1)
    z_relay(zm, zp, 2)
    cross(0)
    z_relay(zm, zp, 3)
    row_push(zp, 3, yn)
    complete(a, plus)
    complete(b, minus)
    rest(zp, (0, 2))
    rest(zm, (1, 3))
    row_push(zm, 3, yn)
    turn(zp)
    turn(zm)
    from_y(0)
    complete(opp, ())
    peer_side(0, 1, 2, 3, yi=yh)
    cross(1)
    to_peer(yc)
    multiply((tn, zp), near, True)
    from_y(1)
    rest(zo, range(4))
    row_push(zo, 3, yn)
    x_relay(ca, cb, 0)
    from_y(2)
    z_relay(yzm, yzp, 0)
    turn(zo)
    multiply((zm, zo), near)
    z_relay(yzm, yzp, 1)
    x_relay(ca, cb, 1)
    row_wait(yn, 3)
    turn(yn)
    multiply((yn,), near)
    complete(ca, plus)
    complete(cb, minus)
    peer_side(0, 3, yi=oy)
    multiply((tn, zp, zm, zo, yn), mid)
    z_relay(yzm, yzp, 2)
    complete(copp, ())
    rest(yzp, (0, 2, 3))
    turn(yzp)
    rest(yzm, (1, 3))
    turn(yzm)
    multiply((yzp, yzm), (0, 12))
    peer_side(1, 2, yi=oy)
    multiply((tn, zp, zm, zo, yn, yzp, yzm), far)
    rest(yzo, range(4))
    turn(yzo)
    multiply((yzo,), (0, 16))

    for item in started:
        if isinstance(item, tuple):
            remote, owner = item

            @pl.when(owner != dp)
            def _():
                remote.wait_send()
        else:
            item.wait_send()


def local(grad_out, down_weight, gate_pre, up_pre):
    tokens, hidden = gate_pre.shape
    depth = grad_out.shape[1]
    sub, rows = tokens // TN, hidden // 2
    return tuple(
        pl.pallas_call(
            factor_kernel,
            out_shape=(
                pltpu.VMEM((rows, hidden), jnp.float32),
                pltpu.VMEM((tokens, hidden), jnp.bfloat16),
            ),
            in_specs=[pl.BlockSpec(memory_space=pl.ANY)] * 4,
            out_specs=(
                pl.BlockSpec(memory_space=pltpu.VMEM),
                pl.BlockSpec(memory_space=pltpu.VMEM),
            ),
            scratch_shapes=[
                pltpu.VMEM((tokens, depth), jnp.bfloat16),
                pltpu.VMEM((hidden, depth), jnp.bfloat16),
                pltpu.VMEM((tokens, hidden), jnp.bfloat16),
                pltpu.VMEM((tokens, hidden), jnp.bfloat16),
                pltpu.VMEM((2, TN, sub, rows), jnp.bfloat16),
                pltpu.VMEM((TN, DP, sub, rows), jnp.bfloat16),
                pltpu.VMEM((DP, tokens, hidden), jnp.bfloat16),
                pltpu.SemaphoreType.DMA((hidden // CHUNK + 3,)),
                pltpu.SemaphoreType.DMA((128,)),
                pltpu.SemaphoreType.DMA((2, TN)),
                pltpu.SemaphoreType.DMA((DP,)),
                pltpu.SemaphoreType.DMA((DP, 4)),
                pltpu.SemaphoreType.DMA((DP // 2,)),
                pltpu.SemaphoreType.DMA((TN, 4)),
            ],
            compiler_params=pltpu.CompilerParams(
                collective_id=0, has_side_effects=True, vmem_limit_bytes=52 * 1024 * 1024
            ),
            name="factor",
        )(grad_out, down_weight, gate_pre, up_pre)
    )


def solution(mesh):
    placed = (P("dp", None), P("tensor", None), P("dp", "tensor"), P("dp", "tensor"))
    return jax.shard_map(
        local,
        mesh=mesh,
        in_specs=placed,
        out_specs=(P("dp", "tensor"), P("dp", "tensor")),
        check_vma=False,
    )
```

```python
import jax
import jax.numpy as jnp
from jax import lax
from jax.experimental import pallas as pl
from jax.experimental.pallas import tpu as pltpu
from jax.sharding import PartitionSpec as P

MESH = pl.DeviceIdType.MESH
NX, NZ = 4, 4
DP, TN = 16, 8
CHUNK = 256
NTILE = 1792
TILES = (512, 512, 512, 256)
PLANE = ((0, 2), (1, 2), (0, 1), (0, 3), (1, 1), (1, 3), (1, 0))
XORDER = (0, 1, 3, 2)


def factor_kernel(
    go_hbm, w_hbm, gate_hbm, up_hbm, out_ref, gu_ref, last, col,
    go, wv, gate, up, s1, rall,
    lin, send, r1, r2, colr, colp, rr,
):
    tokens, hidden = gu_ref.shape
    sub = tokens // TN
    rows = hidden // 2
    half_tok = tokens // 2
    chunks = hidden // CHUNK
    width = DP * sub
    dp = lax.axis_index("dp")
    tn = lax.axis_index("tensor")
    x, yh, c = lax.div(dp, 4), lax.rem(lax.div(dp, 2), 2), lax.rem(dp, 2)
    yl, z = lax.div(tn, NZ), lax.rem(tn, NZ)

    def dp_of(dx, yi, ci):
        return lax.rem(x + dx, NX) * 4 + yi * 2 + ci

    def tn_of(dy, dz):
        return lax.rem(yl + dy, 2) * NZ + lax.rem(z + dz, NZ)

    oy = 1 - yh
    xp, xm = dp_of(1, yh, c), dp_of(3, yh, c)
    yc, peer = dp_of(0, oy, c), dp_of(0, yh, 1 - c)
    zp, zm, yn = tn_of(0, 1), tn_of(0, 3), tn_of(1, 0)

    loads = [pltpu.make_async_copy(go_hbm, go, lin.at[chunks])]
    loads.append(pltpu.make_async_copy(gate_hbm, gate, lin.at[chunks + 1]))
    loads.append(pltpu.make_async_copy(up_hbm, up, lin.at[chunks + 2]))

    def w_load(n):
        rng = pl.ds(pl.multiple_of(n * CHUNK, CHUNK), CHUNK)
        return pltpu.make_async_copy(w_hbm.at[rng], wv.at[rng], lin.at[n])

    loads[0].start()
    w_load(0).start()
    loads[1].start()
    loads[2].start()
    for n in range(1, chunks):
        w_load(n).start()

    barrier = pltpu.get_barrier_semaphore()
    for dy, dz in PLANE:
        pl.semaphore_signal(barrier, inc=1, device_id=(dp, tn_of(dy, dz)), device_id_type=MESH)
    for k in range(1, DP):
        pl.semaphore_signal(barrier, inc=1, device_id=(lax.rem(dp + k, DP), tn), device_id_type=MESH)

    PLANE_SENDS, OWNER_SENDS, COL_SENDS, ROW_SENDS, PEER_SENDS = range(5)
    started = [0] * 5

    def push(kind, src, dst, sem, where):
        started[kind] += 1
        pltpu.make_async_remote_copy(
            src_ref=src,
            dst_ref=dst,
            send_sem=send.at[kind],
            recv_sem=sem,
            device_id=where,
            device_id_type=MESH,
        ).start()

    def arrived(ref, sem):
        pltpu.make_async_copy(ref, ref, sem).wait()

    def quarter(slot, h, k):
        return col.at[slot, pl.ds(k * half_tok, half_tok), pl.ds(h * rows, rows)]

    def col_push(slot, h, k, where):
        ref = quarter(slot, h, k)
        push(COL_SENDS, ref, ref, colr.at[lax.div(slot, 2), 2 * h + k], (where, tn))

    def col_wait(slot, h, k):
        arrived(quarter(slot, h, k), colr.at[lax.div(slot, 2), 2 * h + k])

    def to_peer(slot):
        push(PEER_SENDS, col.at[slot], col.at[slot], colp.at[lax.div(slot, 2)], (peer, tn))

    def from_peer(slot):
        arrived(col.at[slot], colp.at[lax.div(slot, 2)])

    def seg(p, i):
        return rall.at[p, pl.ds(lax.rem(x + XORDER[i], NX) * 4, 4)]

    def row_push(p, i, where):
        push(ROW_SENDS, seg(p, i), seg(p, i), rr.at[p, i], (dp, where))

    def row_wait(p, i):
        arrived(seg(p, i), rr.at[p, i])

    def slice_of(p, h):
        return col.at[dp, pl.ds(pl.multiple_of(p * sub, sub), sub), pl.ds(h * rows, rows)]

    def scatter_plane(h):
        for dy, dz in PLANE:
            p = tn_of(dy, dz)
            push(PLANE_SENDS, slice_of(p, h), s1.at[h, tn], r1.at[h, tn], (dp, p))
        pltpu.make_async_copy(slice_of(tn, h), s1.at[h, tn], r1.at[h, tn]).start()

    def scatter_rows(h):
        for dx in XORDER:
            for yb in range(2):
                t = lax.rem(x + dx, NX) * 2 + yb
                arrived(s1.at[h, t], r1.at[h, t])
                owner = 2 * t + h
                src, dst = s1.at[h, t], rall.at[tn, dp]
                remote = pltpu.make_async_remote_copy(
                    src_ref=src,
                    dst_ref=dst,
                    send_sem=send.at[OWNER_SENDS],
                    recv_sem=r2.at[x],
                    device_id=(owner, tn),
                    device_id_type=MESH,
                )
                local = pltpu.make_async_copy(src, dst, r2.at[x])

                @pl.when(owner != dp)
                def _():
                    remote.start()

                @pl.when(owner == dp)
                def _():
                    local.start()


    def chunk(n):
        w_load(n).wait()
        cols = pl.ds(pl.multiple_of(n * CHUNK, CHUNK), CHUNK)
        grad = lax.dot_general(
            go[...], wv[cols, :], (((1,), (1,)), ((), ())), preferred_element_type=jnp.float32
        )
        g = gate[:, cols].astype(jnp.float32)
        s = 1.0 / (1.0 + jnp.exp(-g))
        gu_ref[:, cols] = (grad * g * s).astype(jnp.bfloat16)
        slope = s * (1.0 + g * (1.0 - s))
        col[dp, :, cols] = (grad * up[:, cols].astype(jnp.float32) * slope).astype(jnp.bfloat16)

    for load in loads:
        load.wait()
    first_half = -(-rows // CHUNK) + 1

    @pl.loop(0, first_half)
    def _(n):
        chunk(n)

    a, b, opp = dp_of(3, yh, c), dp_of(1, yh, c), dp_of(2, yh, c)
    ca, cb, copp = dp_of(3, oy, c), dp_of(1, oy, c), dp_of(2, oy, c)
    yzp, yzm, zo, yzo = tn_of(1, 1), tn_of(1, 3), tn_of(0, 2), tn_of(1, 2)

    def x_relay(left, right, h):
        col_wait(left, h, 0)
        col_push(left, h, 0, xp)
        col_wait(right, h, 1)
        col_push(right, h, 1, xm)

    def gather_rows(i):
        arrived(seg(tn, i), r2.at[lax.rem(x + XORDER[i], NX)])
        row_push(tn, i, zp)
        row_push(tn, i, zm)

    def own_ring(h):
        for k in (0, 1):
            col_push(dp, h, k, xp)
            col_push(dp, h, 1 - k, xm)

    def to_cross(h):
        col_push(dp, h, 0, yc)
        col_push(dp, h, 1, yc)

    def cross(h):
        for k in range(2):
            col_wait(yc, h, k)
        for k in range(2):
            col_push(yc, h, k, xp)
            col_push(yc, h, 1 - k, xm)

    def z_relay(left, right, i):
        if i % 2 == 0:
            row_wait(left, i)
            row_push(left, i, zp)
        else:
            row_wait(right, i)
            row_push(right, i, zm)

    def from_y(i):
        row_wait(yn, i)
        row_push(yn, i, zp)
        row_push(yn, i, zm)

    def rest(p, segments):
        for i in segments:
            row_wait(p, i)

    def complete(slot, done):
        for h in range(2):
            for k in range(2):
                if (h, k) not in done:
                    col_wait(slot, h, k)
        to_peer(slot)

    plus, minus = ((0, 0), (1, 0)), ((0, 1), (1, 1))

    order = [dp_of(dx, yh, ci) for dx in (0, 3, 1, 2) for ci in range(2)]
    order += [dp_of(dx, oy, ci) for dx in (0, 3, 1, 2) for ci in range(2)]
    near, mid, far = (0, 8), (8, 12), (12, 16)
    scale = 1.0 / (DP * tokens)

    def peer_side(*dxs, yi):
        for dx in dxs:
            from_peer(dp_of(dx, yi, 1 - c))

    def turn(p, into=None):
        @pl.loop(0, rows // 128)
        def _(m):
            lanes = pl.ds(pl.multiple_of(m * 128, 128), 128)
            tile = jnp.concatenate([rall[p, s, :, lanes] for s in order], axis=0)
            if into is None:
                wv[lanes, pl.ds(pl.multiple_of(p * width, width), width)] = tile.T
            else:
                into[lanes, :] = tile.T

    def multiply(ps, span, first=False):
        lo, hi = span
        k = (hi - lo) * sub

        @pl.loop(0, hidden // NTILE)
        def _(n):
            cols = pl.ds(pl.multiple_of(n * NTILE, NTILE), NTILE)
            lhs = [
                wv[0:rows, pl.ds(pl.multiple_of(p * width + lo * sub, 128), k)] for p in ps
            ]
            rhs = [
                col[s, pl.ds(pl.multiple_of(p * sub, sub), sub), cols]
                for p in ps
                for s in order[lo:hi]
            ]
            part = scale * jnp.dot(
                jnp.concatenate(lhs, axis=1),
                jnp.concatenate(rhs, axis=0),
                preferred_element_type=jnp.float32,
            )
            if first:
                out_ref[:, cols] = part
            else:
                out_ref[:, cols] += part

    pl.semaphore_wait(barrier, len(PLANE) + DP - 1)
    scatter_plane(0)
    col_push(dp, 0, 0, xp)
    col_push(dp, 0, 1, xm)

    @pl.loop(first_half, chunks)
    def _(n):
        chunk(n)

    scatter_plane(1)
    to_peer(dp)
    scatter_rows(0)
    col_push(dp, 0, 1, xp)
    col_push(dp, 0, 0, xm)
    scatter_rows(1)
    own_ring(1)
    to_cross(0)
    x_relay(a, b, 0)
    gather_rows(0)
    row_push(tn, 0, yn)
    to_cross(1)
    gather_rows(1)
    gather_rows(2)
    gather_rows(3)
    row_push(tn, 1, yn)
    row_push(tn, 2, yn)
    row_push(tn, 3, yn)
    turn(tn)
    z_relay(zm, zp, 0)
    z_relay(zm, zp, 1)
    x_relay(a, b, 1)
    z_relay(zm, zp, 2)
    cross(0)
    z_relay(zm, zp, 3)
    row_push(zp, 3, yn)
    complete(a, plus)
    complete(b, minus)
    rest(zp, (0, 2))
    rest(zm, (1, 3))
    row_push(zm, 3, yn)
    turn(zp)
    turn(zm)
    from_y(0)
    complete(opp, ())
    peer_side(0, 1, 2, 3, yi=yh)
    cross(1)
    to_peer(yc)
    multiply((tn, zp), near, True)
    from_y(1)
    rest(zo, range(4))
    row_push(zo, 3, yn)
    x_relay(ca, cb, 0)
    from_y(2)
    z_relay(yzm, yzp, 0)
    turn(zo)
    multiply((zm, zo), near)
    z_relay(yzm, yzp, 1)
    x_relay(ca, cb, 1)
    row_wait(yn, 3)
    turn(yn)
    multiply((yn,), near)
    complete(ca, plus)
    complete(cb, minus)
    peer_side(0, 3, yi=oy)
    multiply((tn, zp), mid)
    z_relay(yzm, yzp, 2)
    multiply((zm, zo, yn), mid)
    rest(yzp, (0, 2, 3))
    turn(yzp)
    rest(yzm, (1, 3))
    turn(yzm)
    complete(copp, ())
    multiply((yzp, yzm), (0, 12))
    peer_side(1, 2, yi=oy)
    multiply((tn, zp, zm, zo, yn, yzp, yzm), far)
    rest(yzo, range(4))
    turn(yzo, last)

    each = 4
    assert started[COL_SENDS] % each == 0 and started[ROW_SENDS] % each == 0
    arrived(rall.at[0, 0 : started[PLANE_SENDS]], send.at[PLANE_SENDS])
    arrived(rall.at[0, 0 : DP - 1], send.at[OWNER_SENDS])
    arrived(rall.at[0 : started[COL_SENDS] // each], send.at[COL_SENDS])
    arrived(rall.at[0 : started[ROW_SENDS] // each], send.at[ROW_SENDS])
    arrived(col.at[0 : started[PEER_SENDS]], send.at[PEER_SENDS])


def finish_kernel(acc, gu_ref, last, col, out_hbm, gu_hbm, tiles, sem):
    rows, hidden = acc.shape
    tokens = gu_ref.shape[0]
    sub = tokens // TN
    dp = lax.axis_index("dp")
    tn = lax.axis_index("tensor")
    x, yh = lax.div(dp, 4), lax.rem(lax.div(dp, 2), 2)
    p = lax.rem(lax.div(tn, NZ) + 1, 2) * NZ + lax.rem(lax.rem(tn, NZ) + 2, NZ)
    order = [
        lax.rem(x + dx, NX) * 4 + yi * 2 + ci
        for yi in (yh, 1 - yh)
        for dx in (0, 3, 1, 2)
        for ci in range(2)
    ]
    copies = [pltpu.make_async_copy(gu_ref, gu_hbm, sem.at[len(TILES)])]
    copies[0].start()
    first = 0
    for n, size in enumerate(TILES):
        cols = pl.ds(first, size)
        rhs = [col[s, pl.ds(pl.multiple_of(p * sub, sub), sub), cols] for s in order]
        tiles[:, cols] = acc[:, cols] + (1.0 / (DP * tokens)) * jnp.dot(
            last[...],
            jnp.concatenate(rhs, axis=0),
            preferred_element_type=jnp.float32,
        )
        copy = pltpu.make_async_copy(tiles.at[:, cols], out_hbm.at[:, cols], sem.at[n])
        copy.start()
        copies.append(copy)
        first += size
    for copy in copies:
        copy.wait()


def local(grad_out, down_weight, gate_pre, up_pre):
    tokens, hidden = gate_pre.shape
    depth = grad_out.shape[1]
    sub, rows = tokens // TN, hidden // 2
    vmem = pl.BlockSpec(memory_space=pltpu.VMEM)
    anywhere = pl.BlockSpec(memory_space=pl.ANY)
    held = pl.pallas_call(
        factor_kernel,
        out_shape=(
            pltpu.VMEM((rows, hidden), jnp.float32),
            pltpu.VMEM((tokens, hidden), jnp.bfloat16),
            pltpu.VMEM((rows, DP * sub), jnp.bfloat16),
            pltpu.VMEM((DP, tokens, hidden), jnp.bfloat16),
        ),
        in_specs=[anywhere] * 4,
        out_specs=(vmem,) * 4,
        scratch_shapes=[
            pltpu.VMEM((tokens, depth), jnp.bfloat16),
            pltpu.VMEM((hidden, depth), jnp.bfloat16),
            pltpu.VMEM((tokens, hidden), jnp.bfloat16),
            pltpu.VMEM((tokens, hidden), jnp.bfloat16),
            pltpu.VMEM((2, TN, sub, rows), jnp.bfloat16),
            pltpu.VMEM((TN, DP, sub, rows), jnp.bfloat16),
            pltpu.SemaphoreType.DMA((hidden // CHUNK + 3,)),
            pltpu.SemaphoreType.DMA((5,)),
            pltpu.SemaphoreType.DMA((2, TN)),
            pltpu.SemaphoreType.DMA((NX,)),
            pltpu.SemaphoreType.DMA((DP // 2, 4)),
            pltpu.SemaphoreType.DMA((DP // 2,)),
            pltpu.SemaphoreType.DMA((TN, 4)),
        ],
        compiler_params=pltpu.CompilerParams(
            collective_id=0, has_side_effects=True, vmem_limit_bytes=34 * 1024 * 1024
        ),
        name="factor",
    )(grad_out, down_weight, gate_pre, up_pre)
    return tuple(
        pl.pallas_call(
            finish_kernel,
            out_shape=(
                jax.ShapeDtypeStruct((rows, hidden), jnp.float32),
                jax.ShapeDtypeStruct((tokens, hidden), jnp.bfloat16),
            ),
            in_specs=[vmem] * 4,
            out_specs=(anywhere,) * 2,
            scratch_shapes=[
                pltpu.VMEM((rows, hidden), jnp.float32),
                pltpu.SemaphoreType.DMA((len(TILES) + 1,)),
            ],
            compiler_params=pltpu.CompilerParams(vmem_limit_bytes=12 * 1024 * 1024),
            name="finish",
        )(*held)
    )


def solution(mesh):
    placed = (P("dp", None), P("tensor", None), P("dp", "tensor"), P("dp", "tensor"))
    return jax.shard_map(
        local,
        mesh=mesh,
        in_specs=placed,
        out_specs=(P("dp", "tensor"), P("dp", "tensor")),
        check_vma=False,
    )
```

```python
import jax
import jax.numpy as jnp
from jax import lax
from jax.experimental import pallas as pl
from jax.experimental.pallas import tpu as pltpu
from jax.sharding import PartitionSpec as P

MESH = pl.DeviceIdType.MESH
NX, NZ = 4, 4
DP, TN = 16, 8
CHUNK = 256
NTILE = 1792
TILES = (512, 512, 512, 256)
PLANE = ((0, 2), (1, 2), (0, 1), (0, 3), (1, 1), (1, 3), (1, 0))
XORDER = (0, 1, 3, 2)


def factor_kernel(
    go_hbm, w_hbm, gate_hbm, up_hbm, out_ref, gu_ref, last, col,
    go, wv, gate, up, s1, rall,
    lin, send, r1, r2, colr, colp, colq, rr,
):
    tokens, hidden = gu_ref.shape
    sub = tokens // TN
    rows = hidden // 2
    half_tok = tokens // 2
    chunks = hidden // CHUNK
    width = DP * sub
    dp = lax.axis_index("dp")
    tn = lax.axis_index("tensor")
    x, yh, c = lax.div(dp, 4), lax.rem(lax.div(dp, 2), 2), lax.rem(dp, 2)
    yl, z = lax.div(tn, NZ), lax.rem(tn, NZ)

    def dp_of(dx, yi, ci):
        return lax.rem(x + dx, NX) * 4 + yi * 2 + ci

    def tn_of(dy, dz):
        return lax.rem(yl + dy, 2) * NZ + lax.rem(z + dz, NZ)

    oy = 1 - yh
    xp, xm = dp_of(1, yh, c), dp_of(3, yh, c)
    yc, peer = dp_of(0, oy, c), dp_of(0, yh, 1 - c)
    zp, zm, yn = tn_of(0, 1), tn_of(0, 3), tn_of(1, 0)

    loads = [pltpu.make_async_copy(go_hbm, go, lin.at[chunks])]
    loads.append(pltpu.make_async_copy(gate_hbm, gate, lin.at[chunks + 1]))
    loads.append(pltpu.make_async_copy(up_hbm, up, lin.at[chunks + 2]))

    def w_load(n):
        rng = pl.ds(pl.multiple_of(n * CHUNK, CHUNK), CHUNK)
        return pltpu.make_async_copy(w_hbm.at[rng], wv.at[rng], lin.at[n])

    loads[0].start()
    w_load(0).start()
    loads[1].start()
    loads[2].start()
    for n in range(1, chunks):
        w_load(n).start()

    barrier = pltpu.get_barrier_semaphore()
    for dy, dz in PLANE:
        pl.semaphore_signal(barrier, inc=1, device_id=(dp, tn_of(dy, dz)), device_id_type=MESH)
    for k in range(1, DP):
        pl.semaphore_signal(barrier, inc=1, device_id=(lax.rem(dp + k, DP), tn), device_id_type=MESH)

    PLANE_SENDS, OWNER_SENDS, COL_SENDS, ROW_SENDS, PEER_SENDS = range(5)
    started = [0] * 5

    def push(kind, src, dst, sem, where):
        started[kind] += 1
        pltpu.make_async_remote_copy(
            src_ref=src,
            dst_ref=dst,
            send_sem=send.at[kind],
            recv_sem=sem,
            device_id=where,
            device_id_type=MESH,
        ).start()

    def arrived(ref, sem):
        pltpu.make_async_copy(ref, ref, sem).wait()

    def quarter(slot, h, k):
        return col.at[slot, pl.ds(k * half_tok, half_tok), pl.ds(h * rows, rows)]

    def col_push(slot, h, k, where):
        ref = quarter(slot, h, k)
        push(COL_SENDS, ref, ref, colr.at[lax.div(slot, 2), 2 * h + k], (where, tn))

    def col_wait(slot, h, k):
        arrived(quarter(slot, h, k), colr.at[lax.div(slot, 2), 2 * h + k])

    def to_peer(slot):
        push(PEER_SENDS, col.at[slot], col.at[slot], colp.at[lax.div(slot, 2)], (peer, tn))

    def last_to_peer(slot):
        for h in range(2):
            for k in range(2):
                col_wait(slot, h, k)
                ref = quarter(slot, h, k)
                push(COL_SENDS, ref, ref, colq.at[2 * h + k], (peer, tn))

    def last_from_peer(slot):
        for h in range(2):
            for k in range(2):
                arrived(quarter(slot, h, k), colq.at[2 * h + k])

    def from_peer(slot):
        arrived(col.at[slot], colp.at[lax.div(slot, 2)])

    def seg(p, i):
        return rall.at[p, pl.ds(lax.rem(x + XORDER[i], NX) * 4, 4)]

    def row_push(p, i, where):
        push(ROW_SENDS, seg(p, i), seg(p, i), rr.at[p, i], (dp, where))

    def row_wait(p, i):
        arrived(seg(p, i), rr.at[p, i])

    def slice_of(p, h):
        return col.at[dp, pl.ds(pl.multiple_of(p * sub, sub), sub), pl.ds(h * rows, rows)]

    def scatter_plane(h):
        for dy, dz in PLANE:
            p = tn_of(dy, dz)
            push(PLANE_SENDS, slice_of(p, h), s1.at[h, tn], r1.at[h, tn], (dp, p))
        pltpu.make_async_copy(slice_of(tn, h), s1.at[h, tn], r1.at[h, tn]).start()

    def scatter_rows(h):
        for dx in XORDER:
            for yb in range(2):
                t = lax.rem(x + dx, NX) * 2 + yb
                arrived(s1.at[h, t], r1.at[h, t])
                owner = 2 * t + h
                src, dst = s1.at[h, t], rall.at[tn, dp]
                remote = pltpu.make_async_remote_copy(
                    src_ref=src,
                    dst_ref=dst,
                    send_sem=send.at[OWNER_SENDS],
                    recv_sem=r2.at[x],
                    device_id=(owner, tn),
                    device_id_type=MESH,
                )
                local = pltpu.make_async_copy(src, dst, r2.at[x])

                @pl.when(owner != dp)
                def _():
                    remote.start()

                @pl.when(owner == dp)
                def _():
                    local.start()


    def chunk(n):
        w_load(n).wait()
        cols = pl.ds(pl.multiple_of(n * CHUNK, CHUNK), CHUNK)
        grad = lax.dot_general(
            go[...], wv[cols, :], (((1,), (1,)), ((), ())), preferred_element_type=jnp.float32
        )
        g = gate[:, cols].astype(jnp.float32)
        s = 1.0 / (1.0 + jnp.exp(-g))
        gu_ref[:, cols] = (grad * g * s).astype(jnp.bfloat16)
        slope = s * (1.0 + g * (1.0 - s))
        col[dp, :, cols] = (grad * up[:, cols].astype(jnp.float32) * slope).astype(jnp.bfloat16)

    for load in loads:
        load.wait()
    first_half = -(-rows // CHUNK) + 1

    @pl.loop(0, first_half)
    def _(n):
        chunk(n)

    a, b, opp = dp_of(3, yh, c), dp_of(1, yh, c), dp_of(2, yh, c)
    ca, cb, copp = dp_of(3, oy, c), dp_of(1, oy, c), dp_of(2, oy, c)
    yzp, yzm, zo, yzo = tn_of(1, 1), tn_of(1, 3), tn_of(0, 2), tn_of(1, 2)

    def x_relay(left, right, h):
        col_wait(left, h, 0)
        col_push(left, h, 0, xp)
        col_wait(right, h, 1)
        col_push(right, h, 1, xm)

    def gather_rows(i):
        arrived(seg(tn, i), r2.at[lax.rem(x + XORDER[i], NX)])
        row_push(tn, i, zp)
        row_push(tn, i, zm)

    def own_ring(h):
        for k in (0, 1):
            col_push(dp, h, k, xp)
            col_push(dp, h, 1 - k, xm)

    def to_cross(h):
        col_push(dp, h, 0, yc)
        col_push(dp, h, 1, yc)

    def cross(h):
        for k in range(2):
            col_wait(yc, h, k)
        for k in range(2):
            col_push(yc, h, k, xp)
            col_push(yc, h, 1 - k, xm)

    def z_relay(left, right, i):
        if i % 2 == 0:
            row_wait(left, i)
            row_push(left, i, zp)
        else:
            row_wait(right, i)
            row_push(right, i, zm)

    def from_y(i):
        row_wait(yn, i)
        row_push(yn, i, zp)
        row_push(yn, i, zm)

    def rest(p, segments):
        for i in segments:
            row_wait(p, i)

    def complete(slot, done):
        for h in range(2):
            for k in range(2):
                if (h, k) not in done:
                    col_wait(slot, h, k)
        to_peer(slot)

    plus, minus = ((0, 0), (1, 0)), ((0, 1), (1, 1))

    order = [dp_of(dx, yh, ci) for dx in (0, 3, 1, 2) for ci in range(2)]
    order += [dp_of(0, oy, c), dp_of(0, oy, 1 - c), dp_of(3, oy, c), dp_of(1, oy, c)]
    order += [dp_of(3, oy, 1 - c), dp_of(1, oy, 1 - c), dp_of(2, oy, c), dp_of(2, oy, 1 - c)]
    near, mid, far = (0, 8), (8, 12), (12, 16)
    scale = 1.0 / (DP * tokens)

    def peer_side(*dxs, yi):
        for dx in dxs:
            from_peer(dp_of(dx, yi, 1 - c))

    def turn(p, into=None):
        @pl.loop(0, rows // 128)
        def _(m):
            lanes = pl.ds(pl.multiple_of(m * 128, 128), 128)
            tile = jnp.concatenate([rall[p, s, :, lanes] for s in order], axis=0)
            if into is None:
                wv[lanes, pl.ds(pl.multiple_of(p * width, width), width)] = tile.T
            else:
                into[lanes, :] = tile.T

    def multiply(ps, span, first=False):
        lo, hi = span
        k = (hi - lo) * sub

        @pl.loop(0, hidden // NTILE)
        def _(n):
            cols = pl.ds(pl.multiple_of(n * NTILE, NTILE), NTILE)
            lhs = [
                wv[0:rows, pl.ds(pl.multiple_of(p * width + lo * sub, 128), k)] for p in ps
            ]
            rhs = [
                col[s, pl.ds(pl.multiple_of(p * sub, sub), sub), cols]
                for p in ps
                for s in order[lo:hi]
            ]
            part = scale * jnp.dot(
                jnp.concatenate(lhs, axis=1),
                jnp.concatenate(rhs, axis=0),
                preferred_element_type=jnp.float32,
            )
            if first:
                out_ref[:, cols] = part
            else:
                out_ref[:, cols] += part

    pl.semaphore_wait(barrier, len(PLANE) + DP - 1)
    scatter_plane(0)
    col_push(dp, 0, 0, xp)
    col_push(dp, 0, 1, xm)

    @pl.loop(first_half, chunks)
    def _(n):
        chunk(n)

    scatter_plane(1)
    to_peer(dp)
    scatter_rows(0)
    col_push(dp, 0, 1, xp)
    col_push(dp, 0, 0, xm)
    scatter_rows(1)
    own_ring(1)
    to_cross(0)
    x_relay(a, b, 0)
    gather_rows(0)
    row_push(tn, 0, yn)
    to_cross(1)
    gather_rows(1)
    gather_rows(2)
    gather_rows(3)
    row_push(tn, 1, yn)
    row_push(tn, 2, yn)
    row_push(tn, 3, yn)
    turn(tn)
    z_relay(zm, zp, 0)
    z_relay(zm, zp, 1)
    x_relay(a, b, 1)
    z_relay(zm, zp, 2)
    cross(0)
    z_relay(zm, zp, 3)
    row_push(zp, 3, yn)
    complete(a, plus)
    complete(b, minus)
    rest(zp, (0, 2))
    rest(zm, (1, 3))
    row_push(zm, 3, yn)
    turn(zp)
    turn(zm)
    from_y(0)
    complete(opp, ())
    peer_side(0, 1, 2, 3, yi=yh)
    cross(1)
    to_peer(yc)
    multiply((tn, zp), near, True)
    from_y(1)
    rest(zo, range(4))
    row_push(zo, 3, yn)
    x_relay(ca, cb, 0)
    from_y(2)
    z_relay(yzm, yzp, 0)
    turn(zo)
    multiply((zm, zo), near)
    x_relay(ca, cb, 1)
    z_relay(yzm, yzp, 1)
    row_wait(yn, 3)
    turn(yn)
    multiply((yn,), near)
    complete(ca, plus)
    complete(cb, minus)
    peer_side(0, yi=oy)
    multiply((tn, zp, zm, zo, yn), mid)
    z_relay(yzm, yzp, 2)
    rest(yzp, (0, 2, 3))
    turn(yzp)
    multiply((yzp,), (0, 12))
    rest(yzm, (1, 3))
    turn(yzm)
    last_to_peer(copp)
    multiply((yzm,), (0, 12))
    peer_side(3, 1, yi=oy)
    last_from_peer(dp_of(2, oy, 1 - c))
    multiply((tn, zp, zm, zo, yn, yzp, yzm), far)
    rest(yzo, range(4))
    turn(yzo, last)

    each = 4
    assert started[COL_SENDS] % each == 0 and started[ROW_SENDS] % each == 0
    arrived(rall.at[0, 0 : started[PLANE_SENDS]], send.at[PLANE_SENDS])
    arrived(rall.at[0, 0 : DP - 1], send.at[OWNER_SENDS])
    arrived(rall.at[0 : started[COL_SENDS] // each], send.at[COL_SENDS])
    arrived(rall.at[0 : started[ROW_SENDS] // each], send.at[ROW_SENDS])
    arrived(col.at[0 : started[PEER_SENDS]], send.at[PEER_SENDS])


def finish_kernel(acc, gu_ref, last, col, out_hbm, gu_hbm, tiles, sem):
    rows, hidden = acc.shape
    tokens = gu_ref.shape[0]
    sub = tokens // TN
    dp = lax.axis_index("dp")
    tn = lax.axis_index("tensor")
    x, yh, c = lax.div(dp, 4), lax.rem(lax.div(dp, 2), 2), lax.rem(dp, 2)
    p = lax.rem(lax.div(tn, NZ) + 1, 2) * NZ + lax.rem(lax.rem(tn, NZ) + 2, NZ)
    places = [(dx, yh, ci) for dx in (0, 3, 1, 2) for ci in range(2)]
    places += [(dx, 1 - yh, ci) for dx, ci in ((0, c), (0, 1 - c), (3, c), (1, c))]
    places += [(dx, 1 - yh, ci) for dx, ci in ((3, 1 - c), (1, 1 - c), (2, c), (2, 1 - c))]
    order = [lax.rem(x + dx, NX) * 4 + yi * 2 + ci for dx, yi, ci in places]
    copies = [pltpu.make_async_copy(gu_ref, gu_hbm, sem.at[len(TILES)])]
    copies[0].start()
    first = 0
    for n, size in enumerate(TILES):
        cols = pl.ds(first, size)
        rhs = [col[s, pl.ds(pl.multiple_of(p * sub, sub), sub), cols] for s in order]
        tiles[:, cols] = acc[:, cols] + (1.0 / (DP * tokens)) * jnp.dot(
            last[...],
            jnp.concatenate(rhs, axis=0),
            preferred_element_type=jnp.float32,
        )
        copy = pltpu.make_async_copy(tiles.at[:, cols], out_hbm.at[:, cols], sem.at[n])
        copy.start()
        copies.append(copy)
        first += size
    for copy in copies:
        copy.wait()


def local(grad_out, down_weight, gate_pre, up_pre):
    tokens, hidden = gate_pre.shape
    depth = grad_out.shape[1]
    sub, rows = tokens // TN, hidden // 2
    vmem = pl.BlockSpec(memory_space=pltpu.VMEM)
    anywhere = pl.BlockSpec(memory_space=pl.ANY)
    held = pl.pallas_call(
        factor_kernel,
        out_shape=(
            pltpu.VMEM((rows, hidden), jnp.float32),
            pltpu.VMEM((tokens, hidden), jnp.bfloat16),
            pltpu.VMEM((rows, DP * sub), jnp.bfloat16),
            pltpu.VMEM((DP, tokens, hidden), jnp.bfloat16),
        ),
        in_specs=[anywhere] * 4,
        out_specs=(vmem,) * 4,
        scratch_shapes=[
            pltpu.VMEM((tokens, depth), jnp.bfloat16),
            pltpu.VMEM((hidden, depth), jnp.bfloat16),
            pltpu.VMEM((tokens, hidden), jnp.bfloat16),
            pltpu.VMEM((tokens, hidden), jnp.bfloat16),
            pltpu.VMEM((2, TN, sub, rows), jnp.bfloat16),
            pltpu.VMEM((TN, DP, sub, rows), jnp.bfloat16),
            pltpu.SemaphoreType.DMA((hidden // CHUNK + 3,)),
            pltpu.SemaphoreType.DMA((5,)),
            pltpu.SemaphoreType.DMA((2, TN)),
            pltpu.SemaphoreType.DMA((NX,)),
            pltpu.SemaphoreType.DMA((DP // 2, 4)),
            pltpu.SemaphoreType.DMA((DP // 2,)),
            pltpu.SemaphoreType.DMA((4,)),
            pltpu.SemaphoreType.DMA((TN, 4)),
        ],
        compiler_params=pltpu.CompilerParams(
            collective_id=0, has_side_effects=True, vmem_limit_bytes=34 * 1024 * 1024
        ),
        name="factor",
    )(grad_out, down_weight, gate_pre, up_pre)
    return tuple(
        pl.pallas_call(
            finish_kernel,
            out_shape=(
                jax.ShapeDtypeStruct((rows, hidden), jnp.float32),
                jax.ShapeDtypeStruct((tokens, hidden), jnp.bfloat16),
            ),
            in_specs=[vmem] * 4,
            out_specs=(anywhere,) * 2,
            scratch_shapes=[
                pltpu.VMEM((rows, hidden), jnp.float32),
                pltpu.SemaphoreType.DMA((len(TILES) + 1,)),
            ],
            compiler_params=pltpu.CompilerParams(vmem_limit_bytes=12 * 1024 * 1024),
            name="finish",
        )(*held)
    )


def solution(mesh):
    placed = (P("dp", None), P("tensor", None), P("dp", "tensor"), P("dp", "tensor"))
    return jax.shard_map(
        local,
        mesh=mesh,
        in_specs=placed,
        out_specs=(P("dp", "tensor"), P("dp", "tensor")),
        check_vma=False,
    )
```
